32 devices in a mesh: dp: 16 (over z, y, x), tensor: 2 (over core).
Axes of the slice: x: 2, y: 2, z: 4, core: 2. Of those that a mesh axis runs over, the one named last changes fastest.
Arguments:
- encoded: bfloat16 [8192, 1152], P('dp', 'tensor'), may hold values from -9 to 9
- counts: int32 [128], P('dp'), may hold values from 16 to 64
- win_ids: int32 [128, 64], P('dp'), may hold values from 0 to 31, never falling along the last dimension, each value on 1 to 8 neighbouring positions
- dest_seq: int32 [128], P('dp'), may hold values from 0 to 15, as said below
- dest_slot: int32 [128], P('dp'), may hold values from 0 to 7, as said below
- w_first: bfloat16 [1152, 4608], P(None, 'tensor'), may hold values from -0.3125 to 0.3125
- b_first: float32 [4608], P('tensor'), may hold values from -3 to 3
- w_second: bfloat16 [4608, 2304], P('tensor'), may hold values from -0.1875 to 0.1875
- b_second: float32 [2304], P('tensor'), may hold values from -3 to 3
Outputs:
- projected: bfloat16 [4096, 2304], P('dp', 'tensor')
The draws below stay inside these ranges and needn't reach their ends.
Inputs may be any that keep to these rules, and one draw needn't show every extreme that they name: `dest_seq`: every sequence receives exactly 8 samples, no two of them from the same index of dp. `dest_slot`: the samples that one sequence receives have distinct block offsets.
All inputs are finite; a program needn't handle non-finite values.
Results may differ from the reference program's by a relative error of at most 0.009.
Values may be sent and summed in bfloat16 or wider, within the bound.
A program may use at most 128 MiB of HBM per device.

```python
import math
import jax
import jax.numpy as jnp
import numpy as np
from jax import lax

F = 1152
H = 4608
E = 2304
CAP = 64
BLOCK = 32
MOST = 8
SAMP_DEV = 8
SAMPLES = 128
N_TENSOR = 2


def routing_tables(key):
    base = jax.random.fold_in(key, 11)
    key_outer, key_inner, key_shift, key_slots = jax.random.split(base, 4)
    groups = SAMPLES // SAMP_DEV
    outer_perm = jax.random.permutation(key_outer, groups)
    inner_perm = jax.random.permutation(key_inner, groups)
    shifts = jax.random.permutation(key_shift, groups)[:SAMP_DEV]
    sequence = outer_perm[(inner_perm[:, None] + shifts[None, :]) % groups]
    slot_table = jax.vmap(lambda single: jax.random.permutation(single, SAMP_DEV))(jax.random.split(key_slots, groups))
    slot_ids = slot_table[sequence, jnp.arange(SAMP_DEV)[None, :]]
    return (sequence.reshape(-1).astype(jnp.int32), slot_ids.reshape(-1).astype(jnp.int32))


def draw_dest_seq(key, part):
    return routing_tables(key)[0]


def draw_dest_slot(key, part):
    return routing_tables(key)[1]


def touch_ends(array, rng, least, largest):
    spot = [jax.random.randint(jax.random.fold_in(rng, axis), (), 0, length) for axis, length in enumerate(array.shape)]
    longest = array.shape.index(max(array.shape))
    beside = spot[:longest] + [(spot[longest] + 1) % array.shape[longest]] + spot[longest + 1:]
    return array.at[tuple(spot)].set(least).at[tuple(beside)].set(largest)


def with_spikes(result, stream_key, source, target, blocks, factor):
    owner, partner = [(jnp.arange(result.shape[dim]) // (result.shape[dim] // blocks)).reshape([-1 if axis == dim else 1 for axis in range(result.ndim)]) for dim in (source, target)]
    chosen = jax.random.permutation(stream_key, blocks)[partner]
    strong = (owner == chosen) | (owner == (partner + blocks // 2) % blocks)
    return jnp.where(strong, factor * result, result)


def shard_levels(key, dims, pieces, low, top_value):
    loudness = 1.0
    for dim, blocks in pieces:
        heights = jax.random.uniform(jax.random.fold_in(jax.random.fold_in(key, 6), dim), (blocks,), jnp.float32, low / len(pieces), top_value / len(pieces))
        loudness = loudness * jnp.repeat(jnp.exp(heights), dims[dim] // blocks).reshape((-1,) + (1,) * (len(dims) - 1 - dim))
    return loudness


def length_profile(count, total, most, lean):
    portions = [(1 << 20) // math.isqrt(rank ** lean) + 1 for rank in range(2, count + 1)]
    rest, given = total - most - (count - 1), [1] * (count - 1)
    while rest > 0:
        free = [i for i in range(count - 1) if given[i] < most]
        mass, remaining = sum([portions[i] for i in free]), rest
        for i in free:
            more = min(most - given[i], max(1, remaining * portions[i] // mass), rest)
            given[i] = given[i] + more
            rest = rest - more
    return np.array([most] + given)


def uneven(key, count, total, most, lean):
    if count == 2:
        one = jax.random.randint(key, (), max(1, total - most), min(most, total - 1) + 1)
        return jnp.stack([one, total - one])
    sizes = jnp.asarray(length_profile(count, total, most, lean), jnp.int32)
    pairs = (count - 1) // 2
    donor, sink = sizes[1:1 + 2 * pairs:2], sizes[2:2 + 2 * pairs:2]
    margin = jnp.minimum(donor - 1, most - sink)
    shifted = jax.random.randint(jax.random.fold_in(key, 1), (pairs,), 0, 1 << 20) % (margin + 1)
    sizes = sizes.at[1:1 + 2 * pairs:2].set(donor - shifted).at[2:2 + 2 * pairs:2].set(sink + shifted)
    return sizes[jax.random.permutation(jax.random.fold_in(key, 2), count)]


def bell_draw(own_key, shape, scale, reach, cuts=(), kind=jnp.bfloat16):
    loudness = shard_levels(own_key, shape, cuts, -0.22, 0.18) if cuts else 1.0
    drawn = jax.random.normal(own_key, shape, jnp.float32) * scale * loudness
    return jnp.minimum(jnp.maximum(drawn, -reach), reach).astype(kind)


def heavy_noise(rng, shape, spread, bound, cuts, heavy, held_as=jnp.bfloat16):
    drawn = spread * jax.random.normal(rng, shape, jnp.float32)
    if cuts:
        drawn = drawn * shard_levels(rng, shape, cuts, -0.22, 0.18)
    return jnp.clip(with_spikes(drawn, jax.random.fold_in(rng, 3), *heavy), -bound, bound).astype(held_as)


def setup_inputs(seed: int = 0) -> dict:
    streams_of = jax.random.split(jax.random.key(seed), 10)
    return {
        "encoded": bell_draw(streams_of[0], (SAMPLES * CAP, F), 1.5, 9.0, ((0, 16), (1, 2))),
        "counts": touch_ends(jax.random.randint(streams_of[1], (SAMPLES,), CAP // 4, CAP + 1), jax.random.fold_in(streams_of[1], 1), CAP // 4, CAP).astype(jnp.int32),
        "win_ids": jax.vmap(lambda own: jnp.searchsorted(jnp.cumsum(uneven(own, BLOCK, CAP, MOST, 1)), jnp.arange(CAP), side="right"))(jax.random.split(streams_of[2], SAMPLES)).reshape((SAMPLES, CAP)).astype(jnp.int32),
        "dest_seq": draw_dest_seq(jax.random.fold_in(streams_of[9], 71), 0),
        "dest_slot": draw_dest_slot(jax.random.fold_in(streams_of[9], 71), 0),
        "w_first": bell_draw(streams_of[5], (F, H), (F // 3) ** -0.5, 0.3125, ((1, 2),)),
        "b_first": bell_draw(streams_of[6], (H,), 0.5, 3.0, ((0, 2),), jnp.float32),
        "w_second": heavy_noise(streams_of[7], (H, E), (H // 2) ** -0.5, 0.1875, ((0, 2),), (0, 1, 2, 2.0)),
        "b_second": bell_draw(streams_of[8], (E,), 0.5, 3.0, ((0, 2),), jnp.float32),
    }


def reference(encoded, counts, win_ids, dest_seq, dest_slot, w_first, b_first, w_second, b_second):
    tokens = encoded.reshape(SAMPLES, CAP, F)
    positions = jnp.arange(CAP, dtype=jnp.int32)
    ids_live = jnp.where(positions[None, :] < counts[:, None], win_ids, -1)
    windows = jnp.arange(BLOCK, dtype=jnp.int32)
    onehot = (ids_live[:, None, :] == windows[None, :, None]).astype(jnp.float32)
    number = jnp.sum(onehot, axis=2)
    totals = jnp.einsum("nwc,ncf->nwf", onehot, tokens.astype(jnp.float32))
    pooled = (totals / jnp.maximum(number, 1.0)[:, :, None]).astype(jnp.bfloat16)
    position = (dest_seq * SAMP_DEV + dest_slot).astype(jnp.int32)
    packed = jnp.zeros((SAMPLES, BLOCK, F), jnp.bfloat16).at[position].set(pooled)
    packed = packed.reshape(SAMPLES * BLOCK, F)
    preact = jnp.dot(packed, w_first, preferred_element_type=jnp.float32) + b_first
    hidden = jax.nn.gelu(preact, approximate=True).astype(jnp.bfloat16)
    quota_size = H // N_TENSOR
    running = jnp.zeros((SAMPLES * BLOCK, E), jnp.float32)
    for member in range(N_TENSOR):
        portion = jnp.dot(hidden[:, member * quota_size:(member + 1) * quota_size],
                          w_second[member * quota_size:(member + 1) * quota_size],
                          preferred_element_type=jnp.float32).astype(jnp.bfloat16)
        portion = lax.optimization_barrier(portion)
        running = running + portion.astype(jnp.float32)
    return (running + b_second).astype(jnp.bfloat16)
```

```python
import functools
import math

import jax
import jax.numpy as jnp
from jax import lax
from jax.experimental import pallas as pl
from jax.experimental.pallas import tpu as pltpu
from jax.sharding import PartitionSpec as P

BLOCK = 32
LANES = 128
MESH = pl.DeviceIdType.MESH
UNROLL_MAX = 16


def loop(count, body):
    if count <= UNROLL_MAX:
        for i in range(count):
            body(i)
    else:

        @pl.loop(0, count)
        def _(i):
            body(i)


def col_chunks(width, step):
    return [(lo, min(step, width - lo)) for lo in range(0, width, step)]


def gelu(x):
    c0 = math.sqrt(2.0 / math.pi)
    half = 0.5 * x
    return half + half * jnp.tanh(x * (c0 + (c0 * 0.044715) * (x * x)))


def kernel(
    dims,
    seq_s, slot_s, cnt_s, win_v, b1_v, b2_v, enc_h, w1_h, w2_h,
    out_v,
    enc, w1, w2, outgo, arr, sib, route_src, routes, xbuf, hidden, part_out, part_in,
    load_sem, w1_sem, w2_sem, send_sem, recv_sem, rsend_sem, rrecv_sem, fsend_sem, frecv_sem,
    psend_sem, precv_sem,
):
    groups, samples, cap, feat = dims
    full = feat // LANES
    rem = feat - full * LANES
    me = lax.axis_index("dp")
    core = lax.axis_index("tensor")
    other = 1 - core

    barrier = pltpu.get_barrier_semaphore()
    pl.semaphore_signal(barrier, 1, device_id={"tensor": other}, device_id_type=MESH)

    def greet(i):
        peer = lax.rem(me + 1 + i, groups)
        pl.semaphore_signal(barrier, 1, device_id={"dp": peer}, device_id_type=MESH)

    loop(groups - 1, greet)

    pairs = enc.shape[0]
    enc_copies = [
        pltpu.make_async_copy(enc_h.at[:, p * LANES : (p + 1) * LANES], enc.at[p], load_sem.at[p])
        for p in range(pairs)
    ]
    for copy in enc_copies:
        copy.start()

    wide = full * LANES
    mine = pl.multiple_of(core * feat, 64)
    theirs = pl.multiple_of(other * feat, 64)
    spans = [(mine, 0, wide), (theirs, wide, wide)]
    if rem:
        spans += [
            (pl.multiple_of(core * feat + wide, 64), 2 * wide, rem),
            (pl.multiple_of(other * feat + wide, 64), 2 * wide + rem, rem),
        ]
    w1_copies = [
        pltpu.make_async_copy(w1_h.at[pl.ds(src, size)], w1.at[pl.ds(dst, size)], w1_sem.at[n])
        for n, (src, dst, size) in enumerate(spans)
    ]
    half_out = w2.shape[2]
    w2_copies = [
        pltpu.make_async_copy(
            w2_h.at[:, pl.ds(pl.multiple_of(side * half_out, LANES), half_out)], w2.at[n], w2_sem.at[n]
        )
        for n, side in enumerate((other, core))
    ]
    for copy in w1_copies + w2_copies:
        copy.start()

    lane = lax.broadcasted_iota(jnp.int32, route_src.shape, 1)
    route = jnp.full(route_src.shape, -1, jnp.int32)
    for s in range(samples):
        route = jnp.where(lane == s, seq_s[s] * samples + slot_s[s], route)
    route_src[...] = route
    routes[0] = route

    per = LANES // cap
    windows = lax.broadcasted_iota(jnp.int32, (BLOCK, LANES), 0)
    lanes_at = lax.broadcasted_iota(jnp.int32, (BLOCK, LANES), 1)

    def pool(peer, dst):
        chosen = jnp.int32(0)
        for s in range(1, samples):
            chosen = jnp.where(seq_s[s] == peer, jnp.int32(s), chosen)
        pair = chosen // per
        start = (chosen - pair * per) * cap
        ids = jnp.concatenate([win_v[pl.ds(chosen, 1), :]] * per, axis=1)
        live = (lanes_at >= start) & (lanes_at < start + jnp.minimum(cnt_s[chosen], cap))
        hot = (ids == windows) & live
        hot_f = jnp.where(hot, 1.0, 0.0)
        number = jnp.sum(hot_f, axis=1, keepdims=True)
        total = lax.dot_general(
            hot_f.astype(jnp.bfloat16), enc[pair], (((1,), (1,)), ((), ())),
            preferred_element_type=jnp.float32,
        )
        y = (total * (1.0 / jnp.maximum(number, 1.0))).astype(jnp.bfloat16)
        for c in range(full):
            dst[c * BLOCK : (c + 1) * BLOCK, :] = y[:, c * LANES : (c + 1) * LANES]
        if rem:
            tail = y[:, wide:]
            mid = BLOCK // 2
            dst[full * BLOCK :, :] = jnp.concatenate([tail[:mid], tail[mid:]], axis=1)

    def far_first(i):
        off = (i + 1) // 2
        return groups // 2 + off * (2 * (i % 2) - 1)

    def data_copy(j):
        return pltpu.make_async_remote_copy(
            src_ref=outgo.at[j], dst_ref=arr.at[j], send_sem=send_sem.at[j], recv_sem=recv_sem.at[j],
            device_id={"dp": lax.rem(me + j, groups)}, device_id_type=MESH,
        )

    def route_copy(j):
        return pltpu.make_async_remote_copy(
            src_ref=route_src, dst_ref=routes.at[j], send_sem=rsend_sem.at[j], recv_sem=rrecv_sem.at[j],
            device_id={"dp": lax.rem(me + j, groups)}, device_id_type=MESH,
        )

    def forward(j):
        return pltpu.make_async_remote_copy(
            src_ref=arr.at[j], dst_ref=sib.at[j], send_sem=fsend_sem.at[j], recv_sem=frecv_sem.at[j],
            device_id={"tensor": other}, device_id_type=MESH,
        )

    for copy in enc_copies:
        copy.wait()
    first = far_first(0)
    pool(lax.rem(me + first, groups), outgo.at[first])
    pl.semaphore_wait(barrier, groups)

    def stage(i):
        j_next = far_first(i + 1)
        pool(lax.rem(me + j_next, groups), outgo.at[j_next])
        data_copy(far_first(i)).start()

    loop(groups - 2, stage)
    pool(me, arr.at[0])
    data_copy(far_first(groups - 2)).start()
    loop(groups - 1, lambda i: route_copy(i + 1).start())
    forward(0).start()

    def arrive(i):
        j = far_first(groups - 2 - i)
        data_copy(j).wait_recv()
        forward(j).start()

    loop(groups - 1, arrive)
    loop(groups - 1, lambda i: route_copy(i + 1).wait_recv())

    table = routes[...]
    source = lax.broadcasted_iota(jnp.int32, table.shape, 0)
    picks = [
        jnp.minimum(jnp.sum(jnp.where(table == me * samples + k, source, 0)), groups - 1)
        for k in range(samples)
    ]
    loop(groups, lambda i: forward(i).wait_recv())

    for k in range(samples):
        rows = slice(k * BLOCK, (k + 1) * BLOCK)
        for c in range(full):
            lanes = slice(c * LANES, (c + 1) * LANES)
            xbuf[rows, lanes] = arr[picks[k], c * BLOCK : (c + 1) * BLOCK, :]
            lanes = slice(wide + c * LANES, wide + (c + 1) * LANES)
            xbuf[rows, lanes] = sib[picks[k], c * BLOCK : (c + 1) * BLOCK, :]
        if rem:
            a = arr[picks[k], full * BLOCK :, :]
            b = sib[picks[k], full * BLOCK :, :]
            mid = BLOCK // 2
            lo = k * BLOCK
            xbuf[lo : lo + mid, 2 * wide :] = jnp.concatenate([a[:, :rem], b[:, :rem]], axis=1)
            xbuf[lo + mid : lo + 2 * mid, 2 * wide :] = jnp.concatenate([a[:, rem:], b[:, rem:]], axis=1)

    for copy in w1_copies:
        copy.wait()
    total_rows = samples * BLOCK
    step = min(256, total_rows)

    def first_layer(m):
        rows = pl.ds(m * step, step) if isinstance(m, int) else pl.ds(pl.multiple_of(m * step, step), step)
        for lo, size in col_chunks(w1.shape[1], 256):
            acc = jnp.dot(xbuf[rows, :], w1[:, lo : lo + size], preferred_element_type=jnp.float32)
            hidden[rows, lo : lo + size] = gelu(acc + b1_v[lo : lo + size]).astype(jnp.bfloat16)

    tiles = total_rows // step
    if tiles == 1:
        first_layer(0)
    else:
        pl.loop(0, tiles)(first_layer)
    for copy in w2_copies:
        copy.wait()

    chunks = col_chunks(half_out, 256)

    def part_copy(n):
        lo, size = chunks[n]
        return pltpu.make_async_remote_copy(
            src_ref=part_out.at[:, lo : lo + size], dst_ref=part_in.at[:, lo : lo + size],
            send_sem=psend_sem.at[n], recv_sem=precv_sem.at[n],
            device_id={"tensor": other}, device_id_type=MESH,
        )

    def over_rows(body):
        if tiles == 1:
            body(slice(0, step))
        else:

            @pl.loop(0, tiles)
            def _(m):
                body(pl.ds(pl.multiple_of(m * step, step), step))

    for n, (lo, size) in enumerate(chunks):

        def send_part(rows):
            part_out[rows, lo : lo + size] = jnp.dot(
                hidden[rows, :], w2[0, :, lo : lo + size], preferred_element_type=jnp.float32
            ).astype(jnp.bfloat16)

        over_rows(send_part)
        if n:
            part_copy(n - 1).start()
    for n, (lo, size) in enumerate(chunks):

        def keep_part(rows):
            out_v[rows, lo : lo + size] = jnp.dot(
                hidden[rows, :], w2[1, :, lo : lo + size], preferred_element_type=jnp.float32
            ).astype(jnp.bfloat16)

        over_rows(keep_part)
        if n == 0:
            part_copy(len(chunks) - 1).start()
    for n, (lo, size) in enumerate(chunks):
        part_copy(n).wait_recv()

        def finish(rows):
            lanes = slice(lo, lo + size)
            both = out_v[rows, lanes].astype(jnp.float32) + part_in[rows, lanes].astype(jnp.float32)
            out_v[rows, lanes] = (both + b2_v[lanes]).astype(jnp.bfloat16)

        over_rows(finish)
    loop(groups, lambda i: forward(i).wait_send())

    def drain(i):
        data_copy(i + 1).wait_send()
        route_copy(i + 1).wait_send()

    loop(groups - 1, drain)
    for n in range(len(chunks)):
        part_copy(n).wait_send()


def shards(encoded, counts, win_ids, dest_seq, dest_slot, w_first, b_first, w_second, b_second):
    samples, cap = win_ids.shape
    feat = encoded.shape[1]
    groups = lax.axis_size("dp")
    hid = w_first.shape[1]
    half_out = b_second.shape[0]
    rows = samples * BLOCK
    block_rows = BLOCK * feat // LANES
    chunks = len(col_chunks(half_out, 256))
    vmem = pl.BlockSpec(memory_space=pltpu.VMEM)
    smem = pl.BlockSpec(memory_space=pltpu.SMEM)
    hbm = pl.BlockSpec(memory_space=pltpu.HBM)
    bf16 = jnp.bfloat16
    dma = pltpu.SemaphoreType.DMA
    return pl.pallas_call(
        functools.partial(kernel, (groups, samples, cap, feat)),
        out_shape=jax.ShapeDtypeStruct((rows, half_out), bf16),
        in_specs=[smem, smem, smem, vmem, vmem, vmem, hbm, hbm, hbm],
        out_specs=vmem,
        scratch_shapes=[
            pltpu.VMEM((samples * cap // LANES, feat, LANES), bf16),
            pltpu.VMEM((2 * feat, hid), bf16),
            pltpu.VMEM((2, hid, half_out), bf16),
            pltpu.VMEM((groups, block_rows, LANES), bf16),
            pltpu.VMEM((groups, block_rows, LANES), bf16),
            pltpu.VMEM((groups, block_rows, LANES), bf16),
            pltpu.VMEM((1, LANES), jnp.int32),
            pltpu.VMEM((groups, 1, LANES), jnp.int32),
            pltpu.VMEM((rows, 2 * feat), bf16),
            pltpu.VMEM((rows, hid), bf16),
            pltpu.VMEM((rows, half_out), bf16),
            pltpu.VMEM((rows, half_out), bf16),
            dma((samples * cap // LANES,)), dma((4,)), dma((2,)),
            dma((groups,)), dma((groups,)), dma((groups,)), dma((groups,)), dma((groups,)), dma((groups,)),
            dma((chunks,)), dma((chunks,)),
        ],
        compiler_params=pltpu.CompilerParams(
            collective_id=0, has_side_effects=True, vmem_limit_bytes=60 * 1024 * 1024
        ),
    )(
        dest_seq, dest_slot, counts, win_ids, b_first, b_second, encoded.T, w_first, w_second,
    )


def solution(mesh):
    placed = (
        P("dp", "tensor"), P("dp"), P("dp", None), P("dp"), P("dp"),
        P(None, "tensor"), P("tensor"), P("tensor", None), P("tensor"),
    )
    return jax.shard_map(
        shards, mesh=mesh, in_specs=placed, out_specs=P("dp", "tensor"), check_vma=False
    )
```

```python
import functools
import math

import jax
import jax.numpy as jnp
from jax import lax
from jax.experimental import pallas as pl
from jax.experimental.pallas import tpu as pltpu
from jax.sharding import PartitionSpec as P

BLOCK = 32
LANES = 128
MESH = pl.DeviceIdType.MESH
UNROLL_MAX = 16


def loop(count, body):
    if count <= UNROLL_MAX:
        for i in range(count):
            body(i)
    else:

        @pl.loop(0, count)
        def _(i):
            body(i)


def col_chunks(width, step):
    return [(lo, min(step, width - lo)) for lo in range(0, width, step)]


def gelu(x):
    c0 = math.sqrt(2.0 / math.pi)
    half = 0.5 * x
    return half + half * jnp.tanh(x * (c0 + (c0 * 0.044715) * (x * x)))


def kernel(
    dims,
    seq_s, slot_s, cnt_s, win_v, b1_v, b2_v, enc_h, w1_h, w2_h,
    out_v,
    enc, w1, w2, pooled, outgo, arr, sib, route_src, routes, xbuf, hidden, part_out, part_in,
    load_sem, w1_sem, w2_sem, send_sem, recv_sem, rsend_sem, rrecv_sem, fsend_sem, frecv_sem,
    psend_sem, precv_sem,
):
    groups, samples, cap, feat = dims
    full = feat // LANES
    rem = feat - full * LANES
    me = lax.axis_index("dp")
    core = lax.axis_index("tensor")
    other = 1 - core

    barrier = pltpu.get_barrier_semaphore()
    pl.semaphore_signal(barrier, 1, device_id={"tensor": other}, device_id_type=MESH)

    def greet(i):
        peer = lax.rem(me + 1 + i, groups)
        pl.semaphore_signal(barrier, 1, device_id={"dp": peer}, device_id_type=MESH)

    loop(groups - 1, greet)

    pairs = enc.shape[0]
    enc_copies = [
        pltpu.make_async_copy(enc_h.at[:, p * LANES : (p + 1) * LANES], enc.at[p], load_sem.at[p])
        for p in range(pairs)
    ]
    for copy in enc_copies:
        copy.start()

    wide = full * LANES
    mine = pl.multiple_of(core * feat, 64)
    theirs = pl.multiple_of(other * feat, 64)
    spans = [(mine, 0, wide), (theirs, wide, wide)]
    if rem:
        spans += [
            (pl.multiple_of(core * feat + wide, 64), 2 * wide, rem),
            (pl.multiple_of(other * feat + wide, 64), 2 * wide + rem, rem),
        ]
    w1_copies = [
        pltpu.make_async_copy(w1_h.at[pl.ds(src, size)], w1.at[pl.ds(dst, size)], w1_sem.at[n])
        for n, (src, dst, size) in enumerate(spans)
    ]
    half_out = w2.shape[2]
    w2_copies = [
        pltpu.make_async_copy(
            w2_h.at[:, pl.ds(pl.multiple_of(side * half_out, LANES), half_out)], w2.at[n], w2_sem.at[n]
        )
        for n, side in enumerate((other, core))
    ]
    for copy in w1_copies + w2_copies:
        copy.start()

    lane = lax.broadcasted_iota(jnp.int32, route_src.shape, 1)
    route = jnp.full(route_src.shape, -1, jnp.int32)
    for s in range(samples):
        route = jnp.where(lane == s, seq_s[s] * samples + slot_s[s], route)
    route_src[...] = route
    routes[0] = route

    per = LANES // cap
    windows = lax.broadcasted_iota(jnp.int32, (BLOCK, LANES), 0)
    lanes_at = lax.broadcasted_iota(jnp.int32, (BLOCK, LANES), 1)

    def pool(s):
        pair, part = divmod(s, per)
        start = part * cap
        ids = jnp.concatenate([win_v[s : s + 1, :]] * per, axis=1)
        live = (lanes_at >= start) & (lanes_at < start + jnp.minimum(cnt_s[s], cap))
        hot = jnp.where((ids == windows) & live, 1.0, 0.0)
        number = jnp.sum(hot, axis=1, keepdims=True)
        total = lax.dot_general(
            hot.astype(jnp.bfloat16), enc[pair], (((1,), (1,)), ((), ())),
            preferred_element_type=jnp.float32,
        )
        y = (total * (1.0 / jnp.maximum(number, 1.0))).astype(jnp.bfloat16)
        for c in range(full):
            pooled[s, c * BLOCK : (c + 1) * BLOCK, :] = y[:, c * LANES : (c + 1) * LANES]
        if rem:
            tail = y[:, wide:]
            mid = BLOCK // 2
            pooled[s, full * BLOCK :, :] = jnp.concatenate([tail[:mid], tail[mid:]], axis=1)

    def pick(peer):
        chosen = jnp.int32(0)
        for s in range(1, samples):
            chosen = jnp.where(seq_s[s] == peer, jnp.int32(s), chosen)
        return pooled[chosen]

    half = groups // 2
    mine_base = me // half * half
    far_base = half - mine_base

    def far_first(i):
        far = lax.rem(me + i, half)
        near = lax.rem(me + i + 1, half)
        late = i // half
        peer = (1 - late) * (far_base + far) + late * (mine_base + near)
        return lax.rem(peer - me + groups, groups)

    def far_source(i):
        far = lax.rem(me - i + groups, half)
        near = lax.rem(me - i - 1 + 2 * groups, half)
        late = i // half
        peer = (1 - late) * (far_base + far) + late * (mine_base + near)
        return lax.rem(me - peer + groups, groups)

    def fill(j):
        outgo[j] = pick(lax.rem(me + j, groups))

    def data_copy(j):
        return pltpu.make_async_remote_copy(
            src_ref=outgo.at[j], dst_ref=arr.at[j], send_sem=send_sem.at[j], recv_sem=recv_sem.at[j],
            device_id={"dp": lax.rem(me + j, groups)}, device_id_type=MESH,
        )

    def route_copy(j):
        return pltpu.make_async_remote_copy(
            src_ref=route_src, dst_ref=routes.at[j], send_sem=rsend_sem.at[j], recv_sem=rrecv_sem.at[j],
            device_id={"dp": lax.rem(me + j, groups)}, device_id_type=MESH,
        )

    def forward(j):
        return pltpu.make_async_remote_copy(
            src_ref=arr.at[j], dst_ref=sib.at[j], send_sem=fsend_sem.at[j], recv_sem=frecv_sem.at[j],
            device_id={"tensor": other}, device_id_type=MESH,
        )

    for s in range(samples):
        if s % per == 0:
            enc_copies[s // per].wait()
        pool(s)
    loop(2, lambda i: fill(far_first(i)))
    pl.semaphore_wait(barrier, groups)
    loop(groups - 1, lambda i: route_copy(i + 1).start())

    def stage(i):
        fill(far_first(i + 2))
        data_copy(far_first(i)).start()

    loop(groups - 3, stage)
    arr[0] = pick(me)
    data_copy(far_first(groups - 3)).start()
    data_copy(far_first(groups - 2)).start()
    forward(0).start()

    loop(groups - 1, lambda i: route_copy(i + 1).wait_recv())

    table = routes[...]
    source = lax.broadcasted_iota(jnp.int32, table.shape, 0)
    picks = [
        jnp.minimum(jnp.sum(jnp.where(table == me * samples + k, source, 0)), groups - 1)
        for k in range(samples)
    ]
    def arrive(i):
        j = far_source(i)
        data_copy(j).wait_recv()
        forward(j).start()

    loop(groups - 1, arrive)
    loop(groups, lambda i: forward(i).wait_recv())

    for k in range(samples):
        rows = slice(k * BLOCK, (k + 1) * BLOCK)
        for c in range(full):
            lanes = slice(c * LANES, (c + 1) * LANES)
            xbuf[rows, lanes] = arr[picks[k], c * BLOCK : (c + 1) * BLOCK, :]
            lanes = slice(wide + c * LANES, wide + (c + 1) * LANES)
            xbuf[rows, lanes] = sib[picks[k], c * BLOCK : (c + 1) * BLOCK, :]
        if rem:
            a = arr[picks[k], full * BLOCK :, :]
            b = sib[picks[k], full * BLOCK :, :]
            mid = BLOCK // 2
            lo = k * BLOCK
            xbuf[lo : lo + mid, 2 * wide :] = jnp.concatenate([a[:, :rem], b[:, :rem]], axis=1)
            xbuf[lo + mid : lo + 2 * mid, 2 * wide :] = jnp.concatenate([a[:, rem:], b[:, rem:]], axis=1)

    for copy in w1_copies:
        copy.wait()
    total_rows = samples * BLOCK
    step = min(256, total_rows)

    def first_layer(m):
        rows = pl.ds(m * step, step) if isinstance(m, int) else pl.ds(pl.multiple_of(m * step, step), step)
        for lo, size in col_chunks(w1.shape[1], 768):
            acc = jnp.dot(xbuf[rows, :], w1[:, lo : lo + size], preferred_element_type=jnp.float32)
            hidden[rows, lo : lo + size] = gelu(acc + b1_v[lo : lo + size]).astype(jnp.bfloat16)

    tiles = total_rows // step
    if tiles == 1:
        first_layer(0)
    else:
        pl.loop(0, tiles)(first_layer)
    for copy in w2_copies:
        copy.wait()

    chunks = col_chunks(half_out, 384)

    def part_copy(n):
        lo, size = chunks[n]
        return pltpu.make_async_remote_copy(
            src_ref=part_out.at[:, lo : lo + size], dst_ref=part_in.at[:, lo : lo + size],
            send_sem=psend_sem.at[n], recv_sem=precv_sem.at[n],
            device_id={"tensor": other}, device_id_type=MESH,
        )

    def over_rows(body):
        if tiles == 1:
            body(slice(0, step))
        else:

            @pl.loop(0, tiles)
            def _(m):
                body(pl.ds(pl.multiple_of(m * step, step), step))

    for n, (lo, size) in enumerate(chunks):

        def send_part(rows):
            part_out[rows, lo : lo + size] = jnp.dot(
                hidden[rows, :], w2[0, :, lo : lo + size], preferred_element_type=jnp.float32
            ).astype(jnp.bfloat16)

        over_rows(send_part)
        if n:
            part_copy(n - 1).start()
    for n, (lo, size) in enumerate(chunks):

        def keep_part(rows):
            out_v[rows, lo : lo + size] = jnp.dot(
                hidden[rows, :], w2[1, :, lo : lo + size], preferred_element_type=jnp.float32
            ).astype(jnp.bfloat16)

        over_rows(keep_part)
        if n == 0:
            part_copy(len(chunks) - 1).start()
    for n, (lo, size) in enumerate(chunks):
        part_copy(n).wait_recv()

        def finish(rows):
            lanes = slice(lo, lo + size)
            both = out_v[rows, lanes].astype(jnp.float32) + part_in[rows, lanes].astype(jnp.float32)
            out_v[rows, lanes] = (both + b2_v[lanes]).astype(jnp.bfloat16)

        over_rows(finish)
    loop(groups, lambda i: forward(i).wait_send())

    def drain(i):
        data_copy(i + 1).wait_send()
        route_copy(i + 1).wait_send()

    loop(groups - 1, drain)
    for n in range(len(chunks)):
        part_copy(n).wait_send()


def shards(encoded, counts, win_ids, dest_seq, dest_slot, w_first, b_first, w_second, b_second):
    samples, cap = win_ids.shape
    feat = encoded.shape[1]
    groups = lax.axis_size("dp")
    hid = w_first.shape[1]
    half_out = b_second.shape[0]
    rows = samples * BLOCK
    block_rows = BLOCK * feat // LANES
    chunks = len(col_chunks(half_out, 384))
    vmem = pl.BlockSpec(memory_space=pltpu.VMEM)
    smem = pl.BlockSpec(memory_space=pltpu.SMEM)
    hbm = pl.BlockSpec(memory_space=pltpu.HBM)
    bf16 = jnp.bfloat16
    dma = pltpu.SemaphoreType.DMA
    return pl.pallas_call(
        functools.partial(kernel, (groups, samples, cap, feat)),
        out_shape=jax.ShapeDtypeStruct((rows, half_out), bf16),
        in_specs=[smem, smem, smem, vmem, vmem, vmem, hbm, hbm, hbm],
        out_specs=vmem,
        scratch_shapes=[
            pltpu.VMEM((samples * cap // LANES, feat, LANES), bf16),
            pltpu.VMEM((2 * feat, hid), bf16),
            pltpu.VMEM((2, hid, half_out), bf16),
            pltpu.VMEM((samples, block_rows, LANES), bf16),
            pltpu.VMEM((groups, block_rows, LANES), bf16),
            pltpu.VMEM((groups, block_rows, LANES), bf16),
            pltpu.VMEM((groups, block_rows, LANES), bf16),
            pltpu.VMEM((1, LANES), jnp.int32),
            pltpu.VMEM((groups, 1, LANES), jnp.int32),
            pltpu.VMEM((rows, 2 * feat), bf16),
            pltpu.VMEM((rows, hid), bf16),
            pltpu.VMEM((rows, half_out), bf16),
            pltpu.VMEM((rows, half_out), bf16),
            dma((samples * cap // LANES,)), dma((4,)), dma((2,)),
            dma((groups,)), dma((groups,)), dma((groups,)), dma((groups,)), dma((groups,)), dma((groups,)),
            dma((chunks,)), dma((chunks,)),
        ],
        compiler_params=pltpu.CompilerParams(
            collective_id=0, has_side_effects=True, vmem_limit_bytes=60 * 1024 * 1024
        ),
    )(
        dest_seq, dest_slot, counts, win_ids, b_first, b_second, encoded.T, w_first, w_second,
    )


def solution(mesh):
    placed = (
        P("dp", "tensor"), P("dp"), P("dp", None), P("dp"), P("dp"),
        P(None, "tensor"), P("tensor"), P("tensor", None), P("tensor"),
    )
    return jax.shard_map(
        shards, mesh=mesh, in_specs=placed, out_specs=P("dp", "tensor"), check_vma=False
    )
```
